32 devices in a mesh: group: 4 (over x, core), dp: 8 (over z, y).
Axes of the slice: x: 2, y: 2, z: 4, core: 2. Of those that a mesh axis runs over, the one named last changes fastest.
Arguments:
- param_units: int32 [6], replicated, may hold values from 1 to 144, 384 in all
- first_moment: bfloat16 [3072, 7168], P(('group', 'dp')), may hold values from -1.796875 to 1.796875
- second_moment: bfloat16 [3072, 7168], P(('group', 'dp')), may hold values from 0.0099487305 to 1
- grad_parts: bfloat16 [4, 3072, 7168], P('group', 'dp'), may hold values from -17 to 17, as said below
- weights: bfloat16 [3072, 7168], P('dp', 'group'), may hold values from -6 to 6
Outputs:
- new_first: bfloat16 [3072, 7168], P('dp', 'group')
- new_second: bfloat16 [3072, 7168], P('dp', 'group')
- direction: float32 [3072, 7168], P('dp', 'group')
- grad_rms: float32 [], replicated
The draws below stay inside these ranges and needn't reach their ends.
Inputs may be any that keep to these rules, and one draw needn't show every extreme that they name: `param_units`: 6 counts, each from 1 to 144, summing to 384; the largest is exactly 144. `grad_parts`: entries of one group's partial have scales between exp(-3.2) and exp(1.2) that vary with the block of 32 rows and with the column; entries lie within -17 and 17.
All inputs are finite; a program needn't handle non-finite values.
Results may differ from the reference program's by a relative error of at most 0.012.
Values may be sent and summed in bfloat16 or wider, within the bound.
A program may use at most 128 MiB of HBM per device.

```python
import math
import jax
import jax.numpy as jnp
import numpy as np
from jax import lax

W = 7168
PARAMS = 6
ROWS_DEV = 384
GROUPS = 4
SHARDS = 8
ROWS = 3072


def draw_grad_parts(key, part):
    common_key, noise_key, scale_key = jax.random.split(key, 3)
    blocks = ROWS // 32
    full_shape = (GROUPS, blocks, 32, W)
    common_shape = (1, blocks, 32, W)
    row_place = (jnp.arange(blocks, dtype=jnp.float32) / float(blocks)).reshape(1, blocks, 1, 1)
    col_place = (jnp.arange(W, dtype=jnp.float32) / float(W)).reshape(1, 1, 1, W)
    common_draw = jax.random.normal(common_key, common_shape, jnp.float32)
    own_draw = jax.random.normal(noise_key, full_shape, jnp.float32)
    noise_draw = jnp.clip(0.8 * common_draw + 0.6 * own_draw, -5.0, 5.0)
    jitter = jax.random.uniform(scale_key, (GROUPS, blocks, 1, 1), jnp.float32, -0.2, 0.2)
    log_scale = -3.0 + 2.6 * row_place + 1.2 * col_place + jitter
    return (noise_draw * jnp.exp(log_scale)).reshape(GROUPS, ROWS, W).astype(jnp.bfloat16)


def levels(rng, extent, cuts, smallest, largest):
    def one(position, shards_of):
        draws = jax.random.uniform(jax.random.fold_in(jax.random.fold_in(rng, 6), position), (shards_of,), jnp.float32, smallest / len(cuts), largest / len(cuts))
        return jnp.repeat(jnp.exp(draws), extent[position] // shards_of).reshape((-1,) + (1,) * (len(extent) - position - 1))

    factor_of = one(*cuts[0])
    for cut in cuts[1:]:
        factor_of = factor_of * one(*cut)
    return factor_of


def split_up(number_of, total, reach, lean):
    portions = [(1 << 20) // math.isqrt(standing ** lean) + 1 for standing in range(2, number_of + 1)]
    spare, given = total - reach - (number_of - 1), [1] * (number_of - 1)
    while spare > 0:
        movable = [i for i in range(number_of - 1) if given[i] < reach]
        mass, remaining = sum([portions[i] for i in movable]), spare
        for i in movable:
            extra = min(reach - given[i], max(1, remaining * portions[i] // mass), spare)
            given[i] = given[i] + extra
            spare = spare - extra
    return np.array([reach] + given)


def uneven(stream_key, number_of, total, most, skew):
    if number_of == 2:
        one = jax.random.randint(stream_key, (), max(1, total - most), min(most, total - 1) + 1)
        return jnp.stack([one, total - one])
    sizes = jnp.asarray(split_up(number_of, total, most, skew), jnp.int32)
    pairs = (number_of - 1) // 2
    donor, receiver = sizes[1:1 + 2 * pairs:2], sizes[2:2 + 2 * pairs:2]
    slack = jnp.minimum(donor - 1, most - receiver)
    passed = jax.random.randint(jax.random.fold_in(stream_key, 1), (pairs,), 0, 1 << 20) % (slack + 1)
    sizes = sizes.at[1:1 + 2 * pairs:2].set(donor - passed).at[2:2 + 2 * pairs:2].set(receiver + passed)
    return sizes[jax.random.permutation(jax.random.fold_in(stream_key, 2), number_of)]


def normal_values(stream_key, extent, spread, reach, shards=(), held_as=jnp.bfloat16):
    values = jax.random.normal(stream_key, extent, jnp.float32) * spread
    if len(shards) > 0:
        values = levels(stream_key, extent, shards, -0.22, 0.18) * values
    return jnp.clip(values, min=-reach, max=reach).astype(held_as)


def setup_inputs(seed: int = 0) -> dict:
    keys = jax.random.split(jax.random.key(seed), 6)
    param_units = uneven(keys[0], PARAMS, ROWS_DEV, ROWS_DEV * 3 // 8, 2).astype(jnp.int32)
    first_moment = normal_values(keys[1], (ROWS, W), 0.3, 1.796875, ((0, 32),))
    second_moment = jnp.clip(jnp.exp(math.log(1.0) - 4.61031033 * jax.random.uniform(keys[2], (ROWS, W), jnp.float32) ** levels(keys[2], (ROWS, W), ((0, 32),), -0.2, 0.2)), 0.0099487305, 1.0).astype(jnp.bfloat16)
    grad_parts = draw_grad_parts(jax.random.fold_in(keys[5], 71), 0)
    weights = normal_values(keys[4], (ROWS, W), 1.0, 6.0, ((0, 8), (1, 4)))
    return dict(param_units=param_units, first_moment=first_moment, second_moment=second_moment, grad_parts=grad_parts, weights=weights)


def reference(param_units, first_moment, second_moment, grad_parts, weights):
    unit_count = param_units.astype(jnp.int32)
    offsets = (jnp.cumsum(unit_count) - unit_count).astype(jnp.int32)
    local_rows = jnp.arange(ROWS_DEV, dtype=jnp.int32)
    owners = lax.optimization_barrier(jnp.sum(local_rows[:, None] >= (offsets + unit_count)[None, :], axis=1)).astype(jnp.int32)
    row_units = unit_count[owners]
    row_offsets = offsets[owners]
    within = local_rows - row_offsets
    lane_index = jnp.arange(SHARDS, dtype=jnp.int32)[:, None]
    source = (SHARDS * row_offsets[None, :] + lane_index * row_units[None, :] + within[None, :]).reshape(ROWS).astype(jnp.int32)
    first_rows = jnp.take(first_moment, source, axis=0).astype(jnp.float32)
    second_rows = jnp.take(second_moment, source, axis=0).astype(jnp.float32)
    summed = grad_parts[0].astype(jnp.float32)
    for member in range(1, GROUPS):
        summed = summed + grad_parts[member].astype(jnp.float32)
    grad_rms = jnp.sqrt(jnp.sum(summed * summed) / float(ROWS * W))
    clipped = summed / jnp.maximum(grad_rms, 1.0)
    first_new = 0.9 * first_rows + 0.1 * clipped
    second_new = 0.95 * second_rows + 0.05 * clipped * clipped
    direction = first_new / (jnp.sqrt(second_new) + 1e-08) + 0.1 * weights.astype(jnp.float32)
    return (first_new.astype(jnp.bfloat16), second_new.astype(jnp.bfloat16), direction, grad_rms)
```

```python
import functools

import jax
import jax.numpy as jnp
from jax import lax
from jax.experimental import pallas as pl
from jax.experimental.pallas import tpu as pltpu
from jax.sharding import PartitionSpec as P

beta_first = 0.9
beta_second = 0.95
epsilon = 1e-08
decay_weight = 0.1
LANES = 128


class Plan:
    def __init__(self, groups, shards, tiles):
        self.groups, self.shards, self.tiles = groups, shards, tiles
        self.full, self.rest = tiles // shards, tiles % shards
        self.slots = []
        for moment in range(2):
            self.slots += [(moment, turn) for turn in range(self.full)]
            if self.rest:
                self.slots.append((moment, self.full))

    def partial(self, slot):
        return self.slots[slot][1] == self.full

    def place(self, slot, group, lane):
        moment, turn = self.slots[slot]
        if turn < self.full:
            return turn * self.shards + lane, None
        shift = (self.shards // 2) * moment + (self.shards // 4) * lax.rem(group, 2)
        rank = lax.rem(lane + shift, self.shards)
        return self.full * self.shards + jnp.minimum(rank, self.rest - 1), rank < self.rest


def when(condition, body):
    if condition is None:
        body()
    else:
        pl.when(condition)(body)


def both(first, second):
    return second if first is None else first & second


def await_bytes(ref, sem):
    pltpu.make_async_copy(ref, ref, sem).wait()


def spread_kernel(plan, zero_rows, width_part, first_ref, second_ref, middle_ref, send_sem, recv_sem, own_sem):
    group, lane = lax.axis_index("group"), lax.axis_index("dp")
    groups, shards = plan.groups, plan.shards
    base = (group * shards + lane) * zero_rows
    for slot, (moment, _) in enumerate(plan.slots):
        source = (first_ref, second_ref)[moment]

        def send(step, carry, slot=slot, source=source):
            to_group = lax.rem(group + lax.rem(step, groups), groups)
            to_lane = lax.rem(lane + step // groups, shards)
            tile, exists = plan.place(slot, to_group, to_lane)
            column = pl.multiple_of(to_group * width_part + tile * LANES, LANES)

            def start():
                pltpu.make_async_remote_copy(
                    src_ref=source.at[:, pl.ds(column, LANES)],
                    dst_ref=middle_ref.at[slot, pl.ds(base, zero_rows), :],
                    send_sem=send_sem.at[slot],
                    recv_sem=recv_sem.at[slot],
                    device_id=(to_group, to_lane),
                    device_id_type=pl.DeviceIdType.MESH,
                ).start()

            when(exists, start)
            return carry

        tile, exists = plan.place(slot, group, lane)
        column = pl.multiple_of(group * width_part + tile * LANES, LANES)
        own = pltpu.make_async_copy(
            source.at[:, pl.ds(column, LANES)],
            middle_ref.at[slot, pl.ds(base, zero_rows), :],
            own_sem.at[slot],
        )
        when(exists, own.start)
        lax.fori_loop(1, groups * shards, send, 0)
    for slot in range(len(plan.slots)):
        tile, exists = plan.place(slot, group, lane)
        arrived = middle_ref.at[slot, pl.ds(0, (groups * shards - 1) * zero_rows), :]
        if exists is None:
            await_bytes(arrived, send_sem.at[slot])
        else:
            others = groups * plan.rest
            less = middle_ref.at[slot, pl.ds(0, (others - 1) * zero_rows), :]
            more = middle_ref.at[slot, pl.ds(0, others * zero_rows), :]
            pl.when(exists)(functools.partial(await_bytes, less, send_sem.at[slot]))
            pl.when(~exists)(functools.partial(await_bytes, more, send_sem.at[slot]))

        def finish(slot=slot, arrived=arrived):
            await_bytes(arrived, recv_sem.at[slot])
            await_bytes(middle_ref.at[slot, pl.ds(0, zero_rows), :], own_sem.at[slot])

        when(exists, finish)


def deliver_kernel(plan, rows_local, ordered_ref, first_ref, second_ref, send_sem, recv_sem, own_sem):
    group, lane = lax.axis_index("group"), lax.axis_index("dp")
    shards = plan.shards
    results = (first_ref, second_ref)
    for slot, (moment, _) in enumerate(plan.slots):
        tile, exists = plan.place(slot, group, lane)
        target = results[moment].at[:, pl.ds(pl.multiple_of(tile * LANES, LANES), LANES)]

        def start_slot(slot=slot, moment=moment, target=target):
            pltpu.make_async_copy(
                ordered_ref.at[slot, pl.ds(lane * rows_local, rows_local), :], target, own_sem.at[slot]
            ).start()

            def send(step, carry):
                to_lane = lax.rem(lane + step, shards)
                pltpu.make_async_remote_copy(
                    src_ref=ordered_ref.at[slot, pl.ds(to_lane * rows_local, rows_local), :],
                    dst_ref=target,
                    send_sem=send_sem.at[slot],
                    recv_sem=recv_sem.at[moment],
                    device_id=(group, to_lane),
                    device_id_type=pl.DeviceIdType.MESH,
                ).start()
                return carry

            lax.fori_loop(1, shards, send, 0)

        when(exists, start_slot)
    for slot, (moment, turn) in enumerate(plan.slots):
        tile, exists = plan.place(slot, group, lane)

        def finish_slot(slot=slot):
            await_bytes(ordered_ref.at[slot, pl.ds(0, (shards - 1) * rows_local), :], send_sem.at[slot])
            await_bytes(ordered_ref.at[slot, pl.ds(0, rows_local), :], own_sem.at[slot])

        when(exists, finish_slot)
        if slot + 1 == len(plan.slots) or plan.slots[slot + 1][0] != moment:
            result = results[moment]

            def arrive(own, result=result, moment=moment):
                await_bytes(result.at[:, pl.ds(0, (plan.tiles - own) * LANES)], recv_sem.at[moment])

            if exists is None:
                arrive(plan.full)
            else:
                pl.when(exists)(functools.partial(arrive, plan.full + 1))
                pl.when(~exists)(functools.partial(arrive, plan.full))


def local(param_units, first_moment, second_moment, grad_parts, weights):
    groups = lax.axis_size("group")
    shards = lax.axis_size("dp")
    rows_local, width_part = weights.shape
    width_full = grad_parts.shape[2]
    zero_rows = first_moment.shape[0]
    rows = rows_local * shards
    plan = Plan(groups, shards, width_part // LANES)
    slots = len(plan.slots)
    anywhere = pl.BlockSpec(memory_space=pl.ANY)
    in_vmem = pl.BlockSpec(memory_space=pltpu.VMEM)

    summed = lax.psum_scatter(
        grad_parts.astype(jnp.float32).astype(jnp.bfloat16),
        "group",
        scatter_dimension=2,
        tiled=True,
    ).astype(jnp.float32)[0]
    square_sum = lax.psum(jnp.sum(summed * summed), ("group", "dp"))
    grad_rms = jnp.sqrt(square_sum / float(rows * width_full))
    clipped = summed / jnp.maximum(grad_rms, 1.0)

    middle = pl.pallas_call(
        functools.partial(spread_kernel, plan, zero_rows, width_part),
        out_shape=jax.ShapeDtypeStruct((slots, rows, LANES), jnp.bfloat16),
        in_specs=[anywhere, anywhere],
        out_specs=anywhere,
        scratch_shapes=[pltpu.SemaphoreType.DMA((slots,))] * 3,
        compiler_params=pltpu.CompilerParams(has_side_effects=True),
        cost_estimate=pl.CostEstimate(flops=0, bytes_accessed=60_000_000, transcendentals=0),
        name="spread",
    )(first_moment, second_moment)

    offsets = jnp.cumsum(param_units) - param_units
    local_rows = jnp.arange(rows_local, dtype=jnp.int32)
    owners = jnp.sum(local_rows[:, None] >= (offsets + param_units)[None, :], axis=1)
    choose = owners[:, None] == jnp.arange(param_units.shape[0])[None, :]
    row_units = jnp.sum(jnp.where(choose, param_units, 0), axis=1)
    row_offsets = jnp.sum(jnp.where(choose, offsets, 0), axis=1)
    lanes = jnp.arange(shards, dtype=jnp.int32)[:, None]
    source = (shards * row_offsets + lanes * row_units + local_rows - row_offsets).reshape(rows)
    ordered = jnp.take(middle, source, axis=1, mode="clip")

    first_rows, second_rows = pl.pallas_call(
        functools.partial(deliver_kernel, plan, rows_local),
        out_shape=[jax.ShapeDtypeStruct((rows_local, width_part), jnp.bfloat16)] * 2,
        in_specs=[anywhere],
        out_specs=[in_vmem, in_vmem],
        scratch_shapes=[
            pltpu.SemaphoreType.DMA((slots,)),
            pltpu.SemaphoreType.DMA((2,)),
            pltpu.SemaphoreType.DMA((slots,)),
        ],
        compiler_params=pltpu.CompilerParams(has_side_effects=True),
        cost_estimate=pl.CostEstimate(flops=0, bytes_accessed=60_000_000, transcendentals=0),
        name="deliver",
    )(ordered)
    first_rows = first_rows.astype(jnp.float32)
    second_rows = second_rows.astype(jnp.float32)
    first_new = beta_first * first_rows + (1.0 - beta_first) * clipped
    second_new = beta_second * second_rows + (1.0 - beta_second) * clipped * clipped
    direction = first_new / (jnp.sqrt(second_new) + epsilon) + decay_weight * weights.astype(
        jnp.float32
    )
    return (first_new.astype(jnp.bfloat16), second_new.astype(jnp.bfloat16), direction, grad_rms)


def solution(mesh):
    in_specs = (
        P(),
        P(("group", "dp"), None),
        P(("group", "dp"), None),
        P("group", "dp", None),
        P("dp", "group"),
    )
    out_specs = (P("dp", "group"), P("dp", "group"), P("dp", "group"), P())
    return jax.shard_map(local, mesh=mesh, in_specs=in_specs, out_specs=out_specs, check_vma=False)
```

```python
import functools

import jax
import jax.numpy as jnp
from jax import lax
from jax.experimental import pallas as pl
from jax.experimental.pallas import tpu as pltpu
from jax.sharding import PartitionSpec as P

beta_first = 0.9
beta_second = 0.95
epsilon = 1e-08
decay_weight = 0.1
LANES = 128
CHUNKS = 4
BLOCK = 16
RUN = 32


class Plan:
    def __init__(self, groups, shards, tiles):
        self.groups, self.shards, self.tiles = groups, shards, tiles
        self.full, self.rest = tiles // shards, tiles % shards
        self.slots = []
        for moment in range(2):
            self.slots += [(moment, turn) for turn in range(self.full)]
            if self.rest:
                self.slots.append((moment, self.full))

    def partial(self, slot):
        return self.slots[slot][1] == self.full

    def place(self, slot, group, lane):
        moment, turn = self.slots[slot]
        if turn < self.full:
            return turn * self.shards + lane, None
        shift = (self.shards // 2) * moment + (self.shards // 4) * lax.rem(group, 2)
        rank = lax.rem(lane + shift, self.shards)
        return self.full * self.shards + jnp.minimum(rank, self.rest - 1), rank < self.rest


def when(condition, body):
    if condition is None:
        body()
    else:
        pl.when(condition)(body)


def both(first, second):
    return second if first is None else first & second


def await_bytes(ref, sem):
    pltpu.make_async_copy(ref, ref, sem).wait()


def spread_kernel(
    plan, zero_rows, width_part, first_ref, second_ref, grad_ref, middle_ref, summed_ref, square_ref,
    pair_ref, mine_ref, across_ref, landed_ref,
    send_sem, recv_sem, own_sem, load_sem, pair_send_sem, pair_recv_sem, across_send_sem, across_recv_sem,
):
    group, lane = lax.axis_index("group"), lax.axis_index("dp")
    groups, shards = plan.groups, plan.shards
    base = (group * shards + lane) * zero_rows
    rows_local = grad_ref.shape[1]
    chunk = rows_local // CHUNKS
    core = lax.rem(group, 2)
    beside, opposite = group + 1 - 2 * core, lax.rem(group + 2, groups)

    def quarter(owner, rows):
        return grad_ref.at[0, rows, pl.ds(pl.multiple_of(owner * width_part, LANES), width_part)]

    def part(place):
        return pl.ds(place * chunk, chunk)

    def load(place, piece):
        return pltpu.make_async_copy(
            quarter((opposite, group)[place], part(piece)),
            mine_ref.at[place, part(piece), :],
            load_sem.at[place, piece],
        )

    def hand(place, piece):
        return pltpu.make_async_remote_copy(
            src_ref=quarter((lax.rem(beside + 2, groups), beside)[place], part(piece)),
            dst_ref=pair_ref.at[place, part(piece), :],
            send_sem=pair_send_sem.at[place, piece],
            recv_sem=pair_recv_sem.at[place, piece],
            device_id=(beside, lane),
            device_id_type=pl.DeviceIdType.MESH,
        )

    def cross(piece):
        return pltpu.make_async_remote_copy(
            src_ref=across_ref.at[part(piece), :],
            dst_ref=landed_ref.at[part(piece), :],
            send_sem=across_send_sem.at[piece],
            recv_sem=across_recv_sem.at[piece],
            device_id=(opposite, lane),
            device_id_type=pl.DeviceIdType.MESH,
        )

    for place in range(2):
        for piece in range(CHUNKS):
            hand(place, piece).start()
            load(place, piece).start()
    for slot, (moment, _) in enumerate(plan.slots):
        source = (first_ref, second_ref)[moment]

        def send(step, carry, slot=slot, source=source):
            to_group = lax.rem(group + lax.rem(step, groups), groups)
            to_lane = lax.rem(lane + step // groups, shards)
            tile, exists = plan.place(slot, to_group, to_lane)
            column = pl.multiple_of(to_group * width_part + tile * LANES, LANES)

            def start():
                pltpu.make_async_remote_copy(
                    src_ref=source.at[:, pl.ds(column, LANES)],
                    dst_ref=middle_ref.at[slot, pl.ds(base, zero_rows), :],
                    send_sem=send_sem.at[slot],
                    recv_sem=recv_sem.at[slot],
                    device_id=(to_group, to_lane),
                    device_id_type=pl.DeviceIdType.MESH,
                ).start()

            when(exists, start)
            return carry

        tile, exists = plan.place(slot, group, lane)
        column = pl.multiple_of(group * width_part + tile * LANES, LANES)
        own = pltpu.make_async_copy(
            source.at[:, pl.ds(column, LANES)],
            middle_ref.at[slot, pl.ds(base, zero_rows), :],
            own_sem.at[slot],
        )
        when(exists, own.start)
        lax.fori_loop(1, groups * shards, send, 0)
        if slot == 0:
            for piece in range(CHUNKS):
                load(0, piece).wait()
                hand(0, piece).wait()

                def add(block, carry, piece=piece):
                    rows = pl.ds(pl.multiple_of(piece * chunk + block * BLOCK, BLOCK), BLOCK)
                    total = mine_ref[0, rows, :].astype(jnp.float32) + pair_ref[0, rows, :].astype(jnp.float32)
                    across_ref[rows, :] = total.astype(jnp.bfloat16)
                    return carry

                lax.fori_loop(0, chunk // BLOCK, add, 0)
                if piece:
                    cross(piece - 1).start()
            for piece in range(CHUNKS):
                load(1, piece).wait()
                hand(1, piece).wait()
            cross(CHUNKS - 1).start()
    squares = jnp.zeros((1, LANES), jnp.float32)
    for piece in range(CHUNKS):
        cross(piece).wait()

        def finish_sum(block, squares, piece=piece):
            rows = pl.ds(pl.multiple_of(piece * chunk + block * BLOCK, BLOCK), BLOCK)
            total = mine_ref[1, rows, :].astype(jnp.float32) + pair_ref[1, rows, :].astype(jnp.float32)
            total = total + landed_ref[rows, :].astype(jnp.float32)
            summed_ref[rows, :] = total
            down = jnp.sum(total * total, axis=0, keepdims=True)
            for tile in range(plan.tiles):
                squares = squares + down[:, tile * LANES : (tile + 1) * LANES]
            return squares

        squares = lax.fori_loop(0, chunk // BLOCK, finish_sum, squares)
    square_ref[...] = jnp.broadcast_to(squares, square_ref.shape)
    for slot in range(len(plan.slots)):
        tile, exists = plan.place(slot, group, lane)
        arrived = middle_ref.at[slot, pl.ds(0, (groups * shards - 1) * zero_rows), :]
        if exists is None:
            await_bytes(arrived, send_sem.at[slot])
        else:
            others = groups * plan.rest
            less = middle_ref.at[slot, pl.ds(0, (others - 1) * zero_rows), :]
            more = middle_ref.at[slot, pl.ds(0, others * zero_rows), :]
            pl.when(exists)(functools.partial(await_bytes, less, send_sem.at[slot]))
            pl.when(~exists)(functools.partial(await_bytes, more, send_sem.at[slot]))

        def finish(slot=slot, arrived=arrived):
            await_bytes(arrived, recv_sem.at[slot])
            await_bytes(middle_ref.at[slot, pl.ds(0, zero_rows), :], own_sem.at[slot])

        when(exists, finish)


def deliver_kernel(
    plan, rows_local, ordered_ref, square_ref, first_ref, second_ref, total_ref, square_all_ref,
    send_sem, recv_sem, own_sem, square_send_sem, square_recv_sem, square_own_sem,
):
    group, lane = lax.axis_index("group"), lax.axis_index("dp")
    groups, shards = plan.groups, plan.shards
    count = groups * shards
    place = square_all_ref.at[group * shards + lane]
    own_square = pltpu.make_async_copy(square_ref, place, square_own_sem)
    own_square.start()

    def tell(step, carry):
        pltpu.make_async_remote_copy(
            src_ref=square_ref,
            dst_ref=place,
            send_sem=square_send_sem,
            recv_sem=square_recv_sem,
            device_id=(lax.rem(group + lax.rem(step, groups), groups), lax.rem(lane + step // groups, shards)),
            device_id_type=pl.DeviceIdType.MESH,
        ).start()
        return carry

    lax.fori_loop(1, count, tell, 0)
    results = (first_ref, second_ref)
    for slot, (moment, _) in enumerate(plan.slots):
        tile, exists = plan.place(slot, group, lane)
        target = results[moment].at[:, pl.ds(pl.multiple_of(tile * LANES, LANES), LANES)]

        def start_slot(slot=slot, moment=moment, target=target):
            pltpu.make_async_copy(
                ordered_ref.at[slot, pl.ds(lane * rows_local, rows_local), :], target, own_sem.at[slot]
            ).start()

            def send(step, carry):
                to_lane = lax.rem(lane + step, shards)
                pltpu.make_async_remote_copy(
                    src_ref=ordered_ref.at[slot, pl.ds(to_lane * rows_local, rows_local), :],
                    dst_ref=target,
                    send_sem=send_sem.at[slot],
                    recv_sem=recv_sem.at[moment],
                    device_id=(group, to_lane),
                    device_id_type=pl.DeviceIdType.MESH,
                ).start()
                return carry

            lax.fori_loop(1, shards, send, 0)

        when(exists, start_slot)
    own_square.wait()
    others = square_all_ref.at[pl.ds(0, count - 1)]
    await_bytes(others, square_send_sem)
    await_bytes(others, square_recv_sem)
    total_ref[...] = jnp.sum(square_all_ref[...], axis=0)
    for slot, (moment, turn) in enumerate(plan.slots):
        tile, exists = plan.place(slot, group, lane)

        def finish_slot(slot=slot):
            await_bytes(ordered_ref.at[slot, pl.ds(0, (shards - 1) * rows_local), :], send_sem.at[slot])
            await_bytes(ordered_ref.at[slot, pl.ds(0, rows_local), :], own_sem.at[slot])

        when(exists, finish_slot)
        if slot + 1 == len(plan.slots) or plan.slots[slot + 1][0] != moment:
            result = results[moment]

            def arrive(own, result=result, moment=moment):
                await_bytes(result.at[:, pl.ds(0, (plan.tiles - own) * LANES)], recv_sem.at[moment])

            if exists is None:
                arrive(plan.full)
            else:
                pl.when(exists)(functools.partial(arrive, plan.full + 1))
                pl.when(~exists)(functools.partial(arrive, plan.full))


def order_kernel(shards, rows_local, units_ref, middle_ref, ordered_ref, plain_ref, moved_ref):
    rows = shards * rows_local
    slots = middle_ref.shape[0]

    def widen(block, carry):
        part = pl.ds(pl.multiple_of(block * RUN, RUN), RUN)
        for slot in range(slots):
            plain_ref[slot, part, :] = middle_ref[slot, part, :].astype(jnp.float32)
        return carry

    lax.fori_loop(0, rows // RUN, widen, 0)

    def one_lane(lane, carry):
        offset = jnp.int32(0)
        for param in range(units_ref.shape[0]):
            units = units_ref[param]
            source = shards * offset + lane * units
            target = lane * rows_local + offset

            def move(block, carry, source=source, target=target):
                for slot in range(slots):
                    moved_ref[slot, pl.ds(target + block * RUN, RUN), :] = plain_ref[
                        slot, pl.ds(source + block * RUN, RUN), :
                    ]
                return carry

            lax.fori_loop(0, (units + RUN - 1) // RUN, move, 0)
            offset = offset + units
        return carry

    lax.fori_loop(0, shards, one_lane, 0)

    def narrow(block, carry):
        part = pl.ds(pl.multiple_of(block * RUN, RUN), RUN)
        for slot in range(slots):
            ordered_ref[slot, part, :] = moved_ref[slot, part, :].astype(jnp.bfloat16)
        return carry

    lax.fori_loop(0, rows // RUN, narrow, 0)


def local(param_units, first_moment, second_moment, grad_parts, weights):
    groups = lax.axis_size("group")
    shards = lax.axis_size("dp")
    rows_local, width_part = weights.shape
    width_full = grad_parts.shape[2]
    zero_rows = first_moment.shape[0]
    rows = rows_local * shards
    plan = Plan(groups, shards, width_part // LANES)
    slots = len(plan.slots)
    anywhere = pl.BlockSpec(memory_space=pl.ANY)
    in_vmem = pl.BlockSpec(memory_space=pltpu.VMEM)

    dma = pltpu.SemaphoreType.DMA
    piece = (rows_local, width_part)
    middle, summed, squares = pl.pallas_call(
        functools.partial(spread_kernel, plan, zero_rows, width_part),
        out_shape=[
            jax.ShapeDtypeStruct((slots, rows, LANES), jnp.bfloat16),
            jax.ShapeDtypeStruct(piece, jnp.float32),
            jax.ShapeDtypeStruct((8, LANES), jnp.float32),
        ],
        in_specs=[anywhere] * 3,
        out_specs=[anywhere, in_vmem, in_vmem],
        scratch_shapes=[
            pltpu.VMEM((2, *piece), jnp.bfloat16),
            pltpu.VMEM((2, *piece), jnp.bfloat16),
            pltpu.VMEM(piece, jnp.bfloat16),
            pltpu.VMEM(piece, jnp.bfloat16),
        ]
        + [dma((slots,))] * 3
        + [dma((2, CHUNKS))] * 3
        + [dma((CHUNKS,))] * 2,
        compiler_params=pltpu.CompilerParams(has_side_effects=True),
        name="spread",
    )(first_moment, second_moment, grad_parts)

    ordered = pl.pallas_call(
        functools.partial(order_kernel, shards, rows_local),
        out_shape=jax.ShapeDtypeStruct((slots, rows, LANES), jnp.bfloat16),
        in_specs=[pl.BlockSpec(memory_space=pltpu.SMEM), in_vmem],
        out_specs=in_vmem,
        scratch_shapes=[pltpu.VMEM((slots, rows + RUN, LANES), jnp.float32)] * 2,
        name="order",
    )(param_units, middle)

    first_rows, second_rows, square_sums = pl.pallas_call(
        functools.partial(deliver_kernel, plan, rows_local),
        out_shape=[jax.ShapeDtypeStruct(piece, jnp.bfloat16)] * 2
        + [jax.ShapeDtypeStruct((8, LANES), jnp.float32)],
        in_specs=[anywhere, in_vmem],
        out_specs=[in_vmem] * 3,
        scratch_shapes=[
            pltpu.VMEM((groups * shards, 8, LANES), jnp.float32),
            dma((slots,)),
            dma((2,)),
            dma((slots,)),
            dma,
            dma,
            dma,
        ],
        compiler_params=pltpu.CompilerParams(has_side_effects=True),
        name="deliver",
    )(ordered, squares)
    grad_rms = jnp.sqrt(jnp.sum(square_sums[0]) / float(rows * width_full))
    clipped = summed / jnp.maximum(grad_rms, 1.0)
    first_rows = first_rows.astype(jnp.float32)
    second_rows = second_rows.astype(jnp.float32)
    first_new = beta_first * first_rows + (1.0 - beta_first) * clipped
    second_new = beta_second * second_rows + (1.0 - beta_second) * clipped * clipped
    direction = first_new / (jnp.sqrt(second_new) + epsilon) + decay_weight * weights.astype(
        jnp.float32
    )
    return (first_new.astype(jnp.bfloat16), second_new.astype(jnp.bfloat16), direction, grad_rms)


def solution(mesh):
    in_specs = (
        P(),
        P(("group", "dp"), None),
        P(("group", "dp"), None),
        P("group", "dp", None),
        P("dp", "group"),
    )
    out_specs = (P("dp", "group"), P("dp", "group"), P("dp", "group"), P())
    return jax.shard_map(local, mesh=mesh, in_specs=in_specs, out_specs=out_specs, check_vma=False)
```

```python
import functools

import jax
import jax.numpy as jnp
from jax import lax
from jax.experimental import pallas as pl
from jax.experimental.pallas import tpu as pltpu
from jax.sharding import PartitionSpec as P

beta_first = 0.9
beta_second = 0.95
epsilon = 1e-08
decay_weight = 0.1
LANES = 128
CHUNKS = 4
BLOCK = 16
RUN = 32


class Plan:
    def __init__(self, groups, shards, tiles):
        self.groups, self.shards, self.tiles = groups, shards, tiles
        self.full, self.rest = tiles // shards, tiles % shards
        self.slots = []
        for moment in range(2):
            self.slots += [(moment, turn) for turn in range(self.full)]
            if self.rest:
                self.slots.append((moment, self.full))

    def partial(self, slot):
        return self.slots[slot][1] == self.full

    def place(self, slot, group, lane):
        moment, turn = self.slots[slot]
        if turn < self.full:
            return turn * self.shards + lane, None
        shift = (self.shards // 2) * moment + (self.shards // 4) * lax.rem(group, 2)
        rank = lax.rem(lane + shift, self.shards)
        return self.full * self.shards + jnp.minimum(rank, self.rest - 1), rank < self.rest


def when(condition, body):
    if condition is None:
        body()
    else:
        pl.when(condition)(body)


def both(first, second):
    return second if first is None else first & second


def await_bytes(ref, sem):
    pltpu.make_async_copy(ref, ref, sem).wait()


def move_kernel(
    plan, zero_rows, width_part, units_ref, first_ref, second_ref, grad_ref,
    summed_ref, total_ref, first_rows_ref, second_rows_ref,
    pair_ref, mine_ref, across_ref, landed_ref, middle_ref, ordered_ref, plain_ref, square_ref, square_all_ref,
    send_sem, recv_sem, own_sem, load_sem, pair_send_sem, pair_recv_sem, across_send_sem, across_recv_sem,
    out_send_sem, out_recv_sem, out_own_sem, square_send_sem, square_recv_sem, square_own_sem,
):
    group, lane = lax.axis_index("group"), lax.axis_index("dp")
    groups, shards = plan.groups, plan.shards
    base = (group * shards + lane) * zero_rows
    rows_local = grad_ref.shape[1]
    chunk = rows_local // CHUNKS
    core = lax.rem(group, 2)
    beside, opposite = group + 1 - 2 * core, lax.rem(group + 2, groups)

    def quarter(owner, rows):
        return grad_ref.at[0, rows, pl.ds(pl.multiple_of(owner * width_part, LANES), width_part)]

    def part(place):
        return pl.ds(place * chunk, chunk)

    def load(place, piece):
        return pltpu.make_async_copy(
            quarter((opposite, group)[place], part(piece)),
            mine_ref.at[place, part(piece), :],
            load_sem.at[place, piece],
        )

    def hand(place, piece):
        return pltpu.make_async_remote_copy(
            src_ref=quarter((lax.rem(beside + 2, groups), beside)[place], part(piece)),
            dst_ref=pair_ref.at[place, part(piece), :],
            send_sem=pair_send_sem.at[place, piece],
            recv_sem=pair_recv_sem.at[place, piece],
            device_id=(beside, lane),
            device_id_type=pl.DeviceIdType.MESH,
        )

    def cross(piece):
        return pltpu.make_async_remote_copy(
            src_ref=across_ref.at[part(piece), :],
            dst_ref=landed_ref.at[part(piece), :],
            send_sem=across_send_sem.at[piece],
            recv_sem=across_recv_sem.at[piece],
            device_id=(opposite, lane),
            device_id_type=pl.DeviceIdType.MESH,
        )

    for place in range(2):
        for piece in range(CHUNKS):
            hand(place, piece).start()
            load(place, piece).start()
    for slot, (moment, _) in enumerate(plan.slots):
        source = (first_ref, second_ref)[moment]

        def send(step, carry, slot=slot, source=source):
            to_group = lax.rem(group + lax.rem(step, groups), groups)
            to_lane = lax.rem(lane + step // groups, shards)
            tile, exists = plan.place(slot, to_group, to_lane)
            column = pl.multiple_of(to_group * width_part + tile * LANES, LANES)

            def start():
                pltpu.make_async_remote_copy(
                    src_ref=source.at[:, pl.ds(column, LANES)],
                    dst_ref=middle_ref.at[slot, pl.ds(base, zero_rows), :],
                    send_sem=send_sem.at[slot],
                    recv_sem=recv_sem.at[slot],
                    device_id=(to_group, to_lane),
                    device_id_type=pl.DeviceIdType.MESH,
                ).start()

            when(exists, start)
            return carry

        tile, exists = plan.place(slot, group, lane)
        column = pl.multiple_of(group * width_part + tile * LANES, LANES)
        own = pltpu.make_async_copy(
            source.at[:, pl.ds(column, LANES)],
            middle_ref.at[slot, pl.ds(base, zero_rows), :],
            own_sem.at[slot],
        )
        when(exists, own.start)
        lax.fori_loop(1, groups * shards, send, 0)
        if slot == 0:
            for piece in range(CHUNKS):
                load(0, piece).wait()
                hand(0, piece).wait()

                def add(block, carry, piece=piece):
                    rows = pl.ds(pl.multiple_of(piece * chunk + block * BLOCK, BLOCK), BLOCK)
                    total = mine_ref[0, rows, :].astype(jnp.float32) + pair_ref[0, rows, :].astype(jnp.float32)
                    across_ref[rows, :] = total.astype(jnp.bfloat16)
                    return carry

                lax.fori_loop(0, chunk // BLOCK, add, 0)
                if piece:
                    cross(piece - 1).start()
            for piece in range(CHUNKS):
                load(1, piece).wait()
                hand(1, piece).wait()
            cross(CHUNKS - 1).start()

    results = (first_rows_ref, second_rows_ref)
    rows = shards * rows_local

    def put_in_order(slot):
        def widen(block, carry):
            part = pl.multiple_of(block * RUN, RUN)
            plain_ref[pl.ds(pl.multiple_of(part + BLOCK, BLOCK), RUN), :] = middle_ref[
                slot, pl.ds(part, RUN), :
            ].astype(jnp.float32)
            return carry

        lax.fori_loop(0, rows // RUN, widen, 0)

        def gather(block, carry):
            begin = pl.multiple_of(block * BLOCK, BLOCK)
            to_lane = begin // rows_local
            within = begin - to_lane * rows_local
            index = lax.broadcasted_iota(jnp.int32, (BLOCK, LANES), 0) + within
            offset = jnp.int32(0)
            value = jnp.zeros((BLOCK, LANES), jnp.float32)
            for param in range(units_ref.shape[0]):
                units = units_ref[param]
                source = shards * offset + to_lane * units + within - offset
                source = jnp.clip(source + BLOCK, 0, rows + BLOCK)
                value = jnp.where(index >= offset, plain_ref[pl.ds(source, BLOCK), :], value)
                offset = offset + units
            ordered_ref[slot, pl.ds(begin, BLOCK), :] = value.astype(jnp.bfloat16)
            return carry

        lax.fori_loop(0, rows // BLOCK, gather, 0)

    def pass_on(slot, moment, tile):
        target = results[moment].at[:, pl.ds(pl.multiple_of(tile * LANES, LANES), LANES)]
        pltpu.make_async_copy(
            ordered_ref.at[slot, pl.ds(pl.multiple_of(lane * rows_local, BLOCK), rows_local), :],
            target,
            out_own_sem.at[slot],
        ).start()

        def send(step, carry):
            to_lane = lax.rem(lane + step, shards)
            pltpu.make_async_remote_copy(
                src_ref=ordered_ref.at[slot, pl.ds(pl.multiple_of(to_lane * rows_local, BLOCK), rows_local), :],
                dst_ref=target,
                send_sem=out_send_sem.at[slot],
                recv_sem=out_recv_sem.at[moment],
                device_id=(group, to_lane),
                device_id_type=pl.DeviceIdType.MESH,
            ).start()
            return carry

        lax.fori_loop(1, shards, send, 0)

    def sum_up():
        squares = jnp.zeros((1, LANES), jnp.float32)
        for piece in range(CHUNKS):
            cross(piece).wait()

            def finish_sum(block, squares, piece=piece):
                rows = pl.ds(pl.multiple_of(piece * chunk + block * BLOCK, BLOCK), BLOCK)
                total = mine_ref[1, rows, :].astype(jnp.float32) + pair_ref[1, rows, :].astype(jnp.float32)
                total = total + landed_ref[rows, :].astype(jnp.float32)
                summed_ref[rows, :] = total
                down = jnp.sum(total * total, axis=0, keepdims=True)
                for tile in range(plan.tiles):
                    squares = squares + down[:, tile * LANES : (tile + 1) * LANES]
                return squares

            squares = lax.fori_loop(0, chunk // BLOCK, finish_sum, squares)
        square_ref[...] = jnp.broadcast_to(squares, square_ref.shape)

    count = groups * shards
    place = square_all_ref.at[group * shards + lane]

    def tell_squares():
        pltpu.make_async_copy(square_ref, place, square_own_sem).start()

        def tell(step, carry):
            pltpu.make_async_remote_copy(
                src_ref=square_ref,
                dst_ref=place,
                send_sem=square_send_sem,
                recv_sem=square_recv_sem,
                device_id=(lax.rem(group + lax.rem(step, groups), groups), lax.rem(lane + step // groups, shards)),
                device_id_type=pl.DeviceIdType.MESH,
            ).start()
            return carry

        lax.fori_loop(1, count, tell, 0)

    last = len(plan.slots) - 1
    for slot, (moment, _) in enumerate(plan.slots):
        if slot == last:
            sum_up()
        tile, exists = plan.place(slot, group, lane)

        def handle(slot=slot, moment=moment, tile=tile):
            await_bytes(middle_ref.at[slot, pl.ds(0, (count - 1) * zero_rows), :], recv_sem.at[slot])
            await_bytes(middle_ref.at[slot, pl.ds(0, zero_rows), :], own_sem.at[slot])
            put_in_order(slot)
            pass_on(slot, moment, tile)

        when(exists, handle)
        if slot == last:
            tell_squares()

    for slot, (moment, _) in enumerate(plan.slots):
        tile, exists = plan.place(slot, group, lane)
        if exists is None:
            await_bytes(middle_ref.at[slot, pl.ds(0, (count - 1) * zero_rows), :], send_sem.at[slot])
        else:
            others = groups * plan.rest
            less = middle_ref.at[slot, pl.ds(0, (others - 1) * zero_rows), :]
            more = middle_ref.at[slot, pl.ds(0, others * zero_rows), :]
            pl.when(exists)(functools.partial(await_bytes, less, send_sem.at[slot]))
            pl.when(~exists)(functools.partial(await_bytes, more, send_sem.at[slot]))

        def finish_slot(slot=slot):
            await_bytes(ordered_ref.at[slot, pl.ds(0, (shards - 1) * rows_local), :], out_send_sem.at[slot])
            await_bytes(ordered_ref.at[slot, pl.ds(0, rows_local), :], out_own_sem.at[slot])

        when(exists, finish_slot)
        if slot == last or plan.slots[slot + 1][0] != moment:
            result = results[moment]

            def arrive(own, result=result, moment=moment):
                await_bytes(result.at[:, pl.ds(0, (plan.tiles - own) * LANES)], out_recv_sem.at[moment])

            if exists is None:
                arrive(plan.full)
            else:
                pl.when(exists)(functools.partial(arrive, plan.full + 1))
                pl.when(~exists)(functools.partial(arrive, plan.full))
    await_bytes(place, square_own_sem)
    others = square_all_ref.at[pl.ds(0, count - 1)]
    await_bytes(others, square_send_sem)
    await_bytes(others, square_recv_sem)
    total_ref[...] = jnp.sum(square_all_ref[...], axis=0)


def local(param_units, first_moment, second_moment, grad_parts, weights):
    groups = lax.axis_size("group")
    shards = lax.axis_size("dp")
    rows_local, width_part = weights.shape
    width_full = grad_parts.shape[2]
    zero_rows = first_moment.shape[0]
    rows = rows_local * shards
    plan = Plan(groups, shards, width_part // LANES)
    slots = len(plan.slots)
    anywhere = pl.BlockSpec(memory_space=pl.ANY)
    in_vmem = pl.BlockSpec(memory_space=pltpu.VMEM)

    dma = pltpu.SemaphoreType.DMA
    piece = (rows_local, width_part)
    summed, square_sums, first_rows, second_rows = pl.pallas_call(
        functools.partial(move_kernel, plan, zero_rows, width_part),
        out_shape=[
            jax.ShapeDtypeStruct(piece, jnp.float32),
            jax.ShapeDtypeStruct((8, LANES), jnp.float32),
            jax.ShapeDtypeStruct(piece, jnp.bfloat16),
            jax.ShapeDtypeStruct(piece, jnp.bfloat16),
        ],
        in_specs=[pl.BlockSpec(memory_space=pltpu.SMEM)] + [anywhere] * 3,
        out_specs=[in_vmem] * 4,
        scratch_shapes=[
            pltpu.VMEM((2, *piece), jnp.bfloat16),
            pltpu.VMEM((2, *piece), jnp.bfloat16),
            pltpu.VMEM(piece, jnp.bfloat16),
            pltpu.VMEM(piece, jnp.bfloat16),
            pltpu.VMEM((slots, rows, LANES), jnp.bfloat16),
            pltpu.VMEM((slots, rows, LANES), jnp.bfloat16),
            pltpu.VMEM((rows + 2 * BLOCK, LANES), jnp.float32),
            pltpu.VMEM((8, LANES), jnp.float32),
            pltpu.VMEM((groups * shards, 8, LANES), jnp.float32),
        ]
        + [dma((slots,))] * 3
        + [dma((2, CHUNKS))] * 3
        + [dma((CHUNKS,))] * 2
        + [dma((slots,)), dma((2,)), dma((slots,)), dma, dma, dma],
        compiler_params=pltpu.CompilerParams(has_side_effects=True),
        name="move",
    )(param_units, first_moment, second_moment, grad_parts)
    grad_rms = jnp.sqrt(jnp.sum(square_sums[0]) / float(rows * width_full))
    clipped = summed / jnp.maximum(grad_rms, 1.0)
    first_rows = first_rows.astype(jnp.float32)
    second_rows = second_rows.astype(jnp.float32)
    first_new = beta_first * first_rows + (1.0 - beta_first) * clipped
    second_new = beta_second * second_rows + (1.0 - beta_second) * clipped * clipped
    direction = first_new / (jnp.sqrt(second_new) + epsilon) + decay_weight * weights.astype(
        jnp.float32
    )
    return (first_new.astype(jnp.bfloat16), second_new.astype(jnp.bfloat16), direction, grad_rms)


def solution(mesh):
    in_specs = (
        P(),
        P(("group", "dp"), None),
        P(("group", "dp"), None),
        P("group", "dp", None),
        P("dp", "group"),
    )
    out_specs = (P("dp", "group"), P("dp", "group"), P("dp", "group"), P())
    return jax.shard_map(local, mesh=mesh, in_specs=in_specs, out_specs=out_specs, check_vma=False)
```

```python
import functools

import jax
import jax.numpy as jnp
from jax import lax
from jax.experimental import pallas as pl
from jax.experimental.pallas import tpu as pltpu
from jax.sharding import PartitionSpec as P

beta_first = 0.9
beta_second = 0.95
epsilon = 1e-08
decay_weight = 0.1
LANES = 128
CHUNKS = 4
BLOCK = 16
RUN = 32


class Plan:
    def __init__(self, groups, shards, tiles):
        self.groups, self.shards, self.tiles = groups, shards, tiles
        self.full, self.rest = tiles // shards, tiles % shards
        self.slots = []
        for moment in range(2):
            self.slots += [(moment, turn) for turn in range(self.full)]
            if self.rest:
                self.slots.append((moment, self.full))

    def partial(self, slot):
        return self.slots[slot][1] == self.full

    def place(self, slot, group, lane):
        moment, turn = self.slots[slot]
        if turn < self.full:
            return turn * self.shards + lane, None
        shift = (self.shards // 2) * moment + (self.shards // 4) * lax.rem(group, 2)
        rank = lax.rem(lane + shift, self.shards)
        return self.full * self.shards + jnp.minimum(rank, self.rest - 1), rank < self.rest


def when(condition, body):
    if condition is None:
        body()
    else:
        pl.when(condition)(body)


def both(first, second):
    return second if first is None else first & second


def await_bytes(ref, sem):
    pltpu.make_async_copy(ref, ref, sem).wait()


def move_kernel(
    plan, capacity, zero_rows, width_part, pack_start, pack_shift, order_start, order_shift, first_ref, second_ref, grad_ref,
    summed_ref, total_ref, first_rows_ref, second_rows_ref,
    pair_ref, mine_ref, across_ref, landed_ref, middle_ref, packed_ref, other_ref, ordered_ref, plain_ref, square_ref, square_all_ref,
    send_sem, recv_sem, own_sem, load_sem, pair_send_sem, pair_recv_sem, across_send_sem, across_recv_sem,
    half_send_sem, half_recv_sem, out_send_sem, out_recv_sem, out_own_sem, square_send_sem, square_recv_sem, square_own_sem,
):
    group, lane = lax.axis_index("group"), lax.axis_index("dp")
    groups, half = plan.groups, plan.shards
    side, member = lane // half, lax.rem(lane, half)
    base = (group * half + member) * zero_rows
    rows_local = grad_ref.shape[1]
    chunk = rows_local // CHUNKS
    core = lax.rem(group, 2)
    beside, opposite = group + 1 - 2 * core, lax.rem(group + 2, groups)

    def quarter(owner, rows):
        return grad_ref.at[0, rows, pl.ds(pl.multiple_of(owner * width_part, LANES), width_part)]

    def part(place):
        return pl.ds(place * chunk, chunk)

    def load(place, piece):
        return pltpu.make_async_copy(
            quarter((opposite, group)[place], part(piece)),
            mine_ref.at[place, part(piece), :],
            load_sem.at[place, piece],
        )

    def hand(place, piece):
        return pltpu.make_async_remote_copy(
            src_ref=quarter((lax.rem(beside + 2, groups), beside)[place], part(piece)),
            dst_ref=pair_ref.at[place, part(piece), :],
            send_sem=pair_send_sem.at[place, piece],
            recv_sem=pair_recv_sem.at[place, piece],
            device_id=(beside, lane),
            device_id_type=pl.DeviceIdType.MESH,
        )

    def cross(piece):
        return pltpu.make_async_remote_copy(
            src_ref=across_ref.at[part(piece), :],
            dst_ref=landed_ref.at[part(piece), :],
            send_sem=across_send_sem.at[piece],
            recv_sem=across_recv_sem.at[piece],
            device_id=(opposite, lane),
            device_id_type=pl.DeviceIdType.MESH,
        )

    for place in range(2):
        for piece in range(CHUNKS):
            hand(place, piece).start()
            load(place, piece).start()
    for slot, (moment, _) in enumerate(plan.slots):
        source = (first_ref, second_ref)[moment]

        def send(step, carry, slot=slot, source=source):
            to_group = lax.rem(group + lax.rem(step, groups), groups)
            to_member = lax.rem(member + step // groups, half)
            tile, exists = plan.place(slot, to_group, to_member)
            column = pl.multiple_of(to_group * width_part + tile * LANES, LANES)

            def start():
                pltpu.make_async_remote_copy(
                    src_ref=source.at[:, pl.ds(column, LANES)],
                    dst_ref=middle_ref.at[slot, pl.ds(base, zero_rows), :],
                    send_sem=send_sem.at[slot],
                    recv_sem=recv_sem.at[slot],
                    device_id=(to_group, side * half + to_member),
                    device_id_type=pl.DeviceIdType.MESH,
                ).start()

            when(exists, start)
            return carry

        tile, exists = plan.place(slot, group, member)
        column = pl.multiple_of(group * width_part + tile * LANES, LANES)
        own = pltpu.make_async_copy(
            source.at[:, pl.ds(column, LANES)],
            middle_ref.at[slot, pl.ds(base, zero_rows), :],
            own_sem.at[slot],
        )
        when(exists, own.start)
        lax.fori_loop(1, groups * half, send, 0)
        if slot == len(plan.slots) - 1:
            for piece in range(CHUNKS):
                load(0, piece).wait()
                hand(0, piece).wait()

                def add(block, carry, piece=piece):
                    rows = pl.ds(pl.multiple_of(piece * chunk + block * BLOCK, BLOCK), BLOCK)
                    total = mine_ref[0, rows, :].astype(jnp.float32) + pair_ref[0, rows, :].astype(jnp.float32)
                    across_ref[rows, :] = total.astype(jnp.bfloat16)
                    return carry

                lax.fori_loop(0, chunk // BLOCK, add, 0)
                if piece:
                    cross(piece - 1).start()
            for piece in range(CHUNKS):
                load(1, piece).wait()
                hand(1, piece).wait()
            cross(CHUNKS - 1).start()

    results = (first_rows_ref, second_rows_ref)
    kept = groups * half * zero_rows

    def widen(source, slot, at, length):
        def step(block, carry):
            part = pl.multiple_of(block * RUN, RUN)
            plain_ref[pl.ds(pl.multiple_of(part + at + BLOCK, BLOCK), RUN), :] = source[
                slot, pl.ds(part, RUN), :
            ].astype(jnp.float32)
            return carry

        lax.fori_loop(0, length // RUN, step, 0)

    def choose(within, starts, shifts, first, count):
        index = lax.broadcasted_iota(jnp.int32, (BLOCK, LANES), 0) + within
        value = jnp.zeros((BLOCK, LANES), jnp.float32)
        for entry in range(count):
            source = jnp.clip(shifts[first + entry] + within + BLOCK, 0, kept + capacity + BLOCK)
            value = jnp.where(index >= starts[first + entry], plain_ref[pl.ds(source, BLOCK), :], value)
        return value.astype(jnp.bfloat16)

    def swap(slot):
        return pltpu.make_async_remote_copy(
            src_ref=packed_ref.at[slot],
            dst_ref=other_ref.at[slot],
            send_sem=half_send_sem.at[slot],
            recv_sem=half_recv_sem.at[slot],
            device_id=(group, (1 - side) * half + member),
            device_id_type=pl.DeviceIdType.MESH,
        )

    def pack(slot):
        await_bytes(middle_ref.at[slot, pl.ds(0, kept - zero_rows), :], recv_sem.at[slot])
        await_bytes(middle_ref.at[slot, pl.ds(0, zero_rows), :], own_sem.at[slot])
        widen(middle_ref, slot, 0, kept)

        def step(block, carry):
            begin = pl.multiple_of(block * BLOCK, BLOCK)
            packed_ref[slot, pl.ds(begin, BLOCK), :] = choose(
                begin, pack_start, pack_shift, 0, pack_start.shape[0]
            )
            return carry

        lax.fori_loop(0, capacity // BLOCK, step, 0)
        swap(slot).start()

    def put_in_order(slot):
        swap(slot).wait()
        widen(middle_ref, slot, 0, kept)
        widen(other_ref, slot, kept, capacity)
        entries = order_start.shape[0] // half

        def step(block, carry):
            begin = pl.multiple_of(block * BLOCK, BLOCK)
            to_member = begin // rows_local
            ordered_ref[slot, pl.ds(begin, BLOCK), :] = choose(
                begin - to_member * rows_local, order_start, order_shift, to_member * entries, entries
            )
            return carry

        lax.fori_loop(0, half * rows_local // BLOCK, step, 0)

    def pass_on(slot, moment, tile):
        target = results[moment].at[:, pl.ds(pl.multiple_of(tile * LANES, LANES), LANES)]
        pltpu.make_async_copy(
            ordered_ref.at[slot, pl.ds(pl.multiple_of(member * rows_local, BLOCK), rows_local), :],
            target,
            out_own_sem.at[slot],
        ).start()

        def send(step, carry):
            to_member = lax.rem(member + step, half)
            pltpu.make_async_remote_copy(
                src_ref=ordered_ref.at[slot, pl.ds(pl.multiple_of(to_member * rows_local, BLOCK), rows_local), :],
                dst_ref=target,
                send_sem=out_send_sem.at[slot],
                recv_sem=out_recv_sem.at[moment],
                device_id=(group, side * half + to_member),
                device_id_type=pl.DeviceIdType.MESH,
            ).start()
            return carry

        lax.fori_loop(1, half, send, 0)

    def sum_up():
        squares = jnp.zeros((1, LANES), jnp.float32)
        for piece in range(CHUNKS):
            cross(piece).wait()

            def finish_sum(block, squares, piece=piece):
                rows = pl.ds(pl.multiple_of(piece * chunk + block * BLOCK, BLOCK), BLOCK)
                total = mine_ref[1, rows, :].astype(jnp.float32) + pair_ref[1, rows, :].astype(jnp.float32)
                total = total + landed_ref[rows, :].astype(jnp.float32)
                summed_ref[rows, :] = total
                down = jnp.sum(total * total, axis=0, keepdims=True)
                for tile in range(plan.tiles):
                    squares = squares + down[:, tile * LANES : (tile + 1) * LANES]
                return squares

            squares = lax.fori_loop(0, chunk // BLOCK, finish_sum, squares)
        square_ref[...] = jnp.broadcast_to(squares, square_ref.shape)

    shards = 2 * half
    count = groups * shards
    place = square_all_ref.at[group * shards + lane]

    def tell_squares():
        pltpu.make_async_copy(square_ref, place, square_own_sem).start()

        def tell(step, carry):
            pltpu.make_async_remote_copy(
                src_ref=square_ref,
                dst_ref=place,
                send_sem=square_send_sem,
                recv_sem=square_recv_sem,
                device_id=(lax.rem(group + lax.rem(step, groups), groups), lax.rem(lane + step // groups, shards)),
                device_id_type=pl.DeviceIdType.MESH,
            ).start()
            return carry

        lax.fori_loop(1, count, tell, 0)

    last = len(plan.slots) - 1
    for slot in range(len(plan.slots)):
        tile, exists = plan.place(slot, group, member)
        when(exists, functools.partial(pack, slot))
    sum_up()
    tell_squares()
    for slot, (moment, _) in enumerate(plan.slots):
        tile, exists = plan.place(slot, group, member)

        def handle(slot=slot, moment=moment, tile=tile):
            put_in_order(slot)
            pass_on(slot, moment, tile)

        when(exists, handle)

    for slot, (moment, _) in enumerate(plan.slots):
        tile, exists = plan.place(slot, group, member)
        if exists is None:
            await_bytes(middle_ref.at[slot, pl.ds(0, kept - zero_rows), :], send_sem.at[slot])
        else:
            others = groups * plan.rest
            less = middle_ref.at[slot, pl.ds(0, (others - 1) * zero_rows), :]
            more = middle_ref.at[slot, pl.ds(0, others * zero_rows), :]
            pl.when(exists)(functools.partial(await_bytes, less, send_sem.at[slot]))
            pl.when(~exists)(functools.partial(await_bytes, more, send_sem.at[slot]))

        def finish_slot(slot=slot):
            await_bytes(ordered_ref.at[slot, pl.ds(0, (half - 1) * rows_local), :], out_send_sem.at[slot])
            await_bytes(ordered_ref.at[slot, pl.ds(0, rows_local), :], out_own_sem.at[slot])

        when(exists, finish_slot)
        if slot == last or plan.slots[slot + 1][0] != moment:
            result = results[moment]

            def arrive(own, result=result, moment=moment):
                await_bytes(result.at[:, pl.ds(0, (plan.tiles - own) * LANES)], out_recv_sem.at[moment])

            if exists is None:
                arrive(plan.full)
            else:
                pl.when(exists)(functools.partial(arrive, plan.full + 1))
                pl.when(~exists)(functools.partial(arrive, plan.full))
    await_bytes(place, square_own_sem)
    others = square_all_ref.at[pl.ds(0, count - 1)]
    await_bytes(others, square_send_sem)
    await_bytes(others, square_recv_sem)
    total_ref[...] = jnp.sum(square_all_ref[...], axis=0)


def make_tables(units, groups, shards, rows_local, zero_rows):
    half = shards // 2
    window = half * zero_rows
    side = lax.axis_index("dp") // half
    params = units.shape[0]
    offsets = jnp.cumsum(units) - units
    window_group = jnp.arange(groups, dtype=jnp.int32)[None, :]

    def runs(from_side):
        begin = (shards * offsets + (1 - from_side) * half * units)[:, None]
        floor = (2 * window_group + from_side) * window
        low = jnp.maximum(begin, floor)
        length = jnp.maximum(jnp.minimum(begin + (half * units)[:, None], floor + window) - low, 0)
        return low, length, floor

    low, length, floor = runs(side)
    held = (low - floor + window_group * window).reshape(-1)
    length = length.reshape(-1)
    start = jnp.cumsum(length) - length
    rank = jnp.where(length > 0, jnp.cumsum((length > 0).astype(jnp.int32)) - 1, -1)
    pick = rank[None, :] == jnp.arange(params + groups - 1, dtype=jnp.int32)[:, None]
    unused = ~jnp.any(pick, axis=1)
    pack_start = jnp.sum(jnp.where(pick, start, 0), axis=1) + jnp.where(unused, shards * rows_local, 0)
    pack_shift = jnp.sum(jnp.where(pick, held - start, 0), axis=1)

    their_low, their_length, _ = runs(1 - side)
    lanes = side * half + jnp.arange(half, dtype=jnp.int32)[:, None]
    row = shards * offsets + lanes * units
    first_part = jnp.minimum(units, (row // window + 1) * window - row)
    row = jnp.stack([row, row + first_part], axis=-1)
    start_at = jnp.stack([jnp.broadcast_to(offsets, first_part.shape), offsets + first_part], axis=-1)
    before = jnp.clip(row[..., None, None] - their_low, 0, their_length)
    packed = jnp.sum(before, axis=(-2, -1)) + groups * window
    which = row // window
    here = which // 2 * window + row % window
    place = jnp.where(which % 2 == side, here, packed)
    tables = (pack_start, pack_shift, start_at.reshape(-1), (place - start_at).reshape(-1))
    return tuple(t.astype(jnp.int32) for t in tables), jnp.sum(length)


def local(param_units, first_moment, second_moment, grad_parts, weights):
    groups = lax.axis_size("group")
    shards = lax.axis_size("dp")
    rows_local, width_part = weights.shape
    width_full = grad_parts.shape[2]
    zero_rows = first_moment.shape[0]
    rows = rows_local * shards
    half = shards // 2
    plan = Plan(groups, half, width_part // LANES)
    slots = len(plan.slots)
    anywhere = pl.BlockSpec(memory_space=pl.ANY)
    in_vmem = pl.BlockSpec(memory_space=pltpu.VMEM)

    dma = pltpu.SemaphoreType.DMA
    piece = (rows_local, width_part)
    tables, crossing = make_tables(param_units, groups, shards, rows_local, zero_rows)

    def run(capacity, *operands):
        return pl.pallas_call(
            functools.partial(move_kernel, plan, capacity, zero_rows, width_part),
            out_shape=[
                jax.ShapeDtypeStruct(piece, jnp.float32),
                jax.ShapeDtypeStruct((8, LANES), jnp.float32),
                jax.ShapeDtypeStruct(piece, jnp.bfloat16),
                jax.ShapeDtypeStruct(piece, jnp.bfloat16),
            ],
            in_specs=[pl.BlockSpec(memory_space=pltpu.SMEM)] * 4 + [anywhere] * 3,
            out_specs=[in_vmem] * 4,
            scratch_shapes=[
                pltpu.VMEM((2, *piece), jnp.bfloat16),
                pltpu.VMEM((2, *piece), jnp.bfloat16),
                pltpu.VMEM(piece, jnp.bfloat16),
                pltpu.VMEM(piece, jnp.bfloat16),
                pltpu.VMEM((slots, rows // 2, LANES), jnp.bfloat16),
                pltpu.VMEM((slots, capacity, LANES), jnp.bfloat16),
                pltpu.VMEM((slots, capacity, LANES), jnp.bfloat16),
                pltpu.VMEM((slots, rows // 2, LANES), jnp.bfloat16),
                pltpu.VMEM((rows // 2 + capacity + 2 * BLOCK, LANES), jnp.float32),
                pltpu.VMEM((8, LANES), jnp.float32),
                pltpu.VMEM((groups * shards, 8, LANES), jnp.float32),
            ]
            + [dma((slots,))] * 3
            + [dma((2, CHUNKS))] * 3
            + [dma((CHUNKS,))] * 2
            + [dma((slots,)), dma((slots,)), dma((slots,)), dma((2,)), dma((slots,)), dma, dma, dma],
            compiler_params=pltpu.CompilerParams(has_side_effects=True),
            name="move",
        )(*operands)

    levels = [rows * part // 24 // RUN * RUN for part in (5, 6, 7, 8)] + [rows // 2]
    level = jnp.sum((crossing > jnp.array(levels[:-1], jnp.int32)).astype(jnp.int32))
    summed, square_sums, first_rows, second_rows = lax.switch(
        level,
        [functools.partial(run, capacity) for capacity in levels],
        *tables, first_moment, second_moment, grad_parts,
    )
    grad_rms = jnp.sqrt(jnp.sum(square_sums[0]) / float(rows * width_full))
    clipped = summed / jnp.maximum(grad_rms, 1.0)
    first_rows = first_rows.astype(jnp.float32)
    second_rows = second_rows.astype(jnp.float32)
    first_new = beta_first * first_rows + (1.0 - beta_first) * clipped
    second_new = beta_second * second_rows + (1.0 - beta_second) * clipped * clipped
    direction = first_new / (jnp.sqrt(second_new) + epsilon) + decay_weight * weights.astype(
        jnp.float32
    )
    return (first_new.astype(jnp.bfloat16), second_new.astype(jnp.bfloat16), direction, grad_rms)


def solution(mesh):
    in_specs = (
        P(),
        P(("group", "dp"), None),
        P(("group", "dp"), None),
        P("group", "dp", None),
        P("dp", "group"),
    )
    out_specs = (P("dp", "group"), P("dp", "group"), P("dp", "group"), P())
    return jax.shard_map(local, mesh=mesh, in_specs=in_specs, out_specs=out_specs, check_vma=False)
```
